32 devices in a mesh: blk: 32 (over z, y, x, core).
Axes of the slice: x: 2, y: 2, z: 4, core: 2. Of those that a mesh axis runs over, the one named last changes fastest.
Arguments:
- node_latent: bfloat16 [131072, 128], P('blk'), may hold values from -16 to 16
- edge_latent: bfloat16 [786432, 128], P('blk'), may hold values from -6 to 6
- edge_ends: int32 [2, 786432], P(None, 'blk'), may hold values from 0 to 5631, as said below
- edge_owned: int32 [786432], P('blk'), may hold values from 0 to 1, as said below
- send_index: int32 [32, 6, 256], P('blk'), may hold values from 0 to 4095, as said below
- edge_w1: bfloat16 [2, 384, 128], replicated, may hold values from -0.3125 to 0.3125
- edge_b1: float32 [2, 128], replicated, may hold values from -3 to 3
- edge_w2: bfloat16 [2, 128, 128], replicated, may hold values from -0.5 to 0.5
- edge_gain: float32 [2, 128], replicated, may hold values from 0.5 to 1.5
- edge_shift: float32 [2, 128], replicated, may hold values from -2 to 2
- node_w1: bfloat16 [2, 256, 128], replicated, may hold values from -0.375 to 0.375
- node_b1: float32 [2, 128], replicated, may hold values from -3 to 3
- node_w2: bfloat16 [2, 128, 128], replicated, may hold values from -0.5 to 0.5
- node_gain: float32 [2, 128], replicated, may hold values from 0.5 to 1.5
- node_shift: float32 [2, 128], replicated, may hold values from -2 to 2
Outputs:
- node_out: bfloat16 [131072, 128], P('blk')
- edge_out: bfloat16 [786432, 128], P('blk')
The draws below stay inside these ranges and needn't reach their ends.
Inputs may be any that keep to these rules, and one draw needn't show every extreme that they name: edge_ends[0] holds each slot's sender, edge_ends[1] its receiver, as entries of the block's extended node list. Slot s of a block lies in tile t = s // 128; each of its ends is either an own node from (t // 6) * 128 to (t // 6 + 1) * 128 - 1 or a halo entry from 4096 + (t % 6) * 256 to 4096 + (t % 6 + 1) * 256 - 1; at most one end of a slot is a halo entry. `edge_owned`: in each block the slots with 1 come first; every block has at least 15360 of them. send_index[b, k] lists 256 distinct nodes of block b.
All inputs are finite; a program needn't handle non-finite values.
Results may differ from the reference program's by a relative error of at most 0.0085.
Values may be sent and summed in bfloat16 or wider, within the bound.
A program may use at most 128 MiB of HBM per device.

```python
import jax
import jax.numpy as jnp
from jax import lax

LATENT = 128
NODE_DEV = 4096
HALO = 256
LAYERS = 2
FACES = 6
GX = 4
GY = 4
EDGE_TILE = 128
EDGE_DEV = 24576
EDGES = 786432
N_BLK = 32


def draw_node_latent(key, part):
    total_rows = NODE_DEV * N_BLK
    position = jnp.arange(total_rows, dtype=jnp.float32)[:, None] / (total_rows - 1)
    values = jnp.clip(jax.random.normal(key, (total_rows, LATENT), jnp.float32), -5.0, 5.0)
    scales = 1.0 + 2.0 * position
    return (values * scales).astype(jnp.bfloat16)


def draw_edge_ends(key, part):
    total_slots = EDGE_DEV * N_BLK
    subkeys = jax.random.split(jax.random.fold_in(key, 11), 4)
    slot = jnp.arange(total_slots, dtype=jnp.int32) % EDGE_DEV
    tile_id = slot // EDGE_TILE
    own_base = tile_id // FACES * EDGE_TILE
    halo_base = NODE_DEV + tile_id % FACES * HALO
    categories = jax.random.randint(subkeys[0], (total_slots,), 0, 8)
    first_local = jax.random.randint(subkeys[1], (total_slots,), 0, EDGE_TILE)
    step_by = jax.random.randint(subkeys[2], (total_slots,), 1, EDGE_TILE)
    second_local = (first_local + step_by) % EDGE_TILE
    remote = halo_base + jax.random.randint(subkeys[3], (total_slots,), 0, HALO)
    senders = jnp.where(categories < 2, remote, own_base + first_local)
    receivers = jnp.where((categories >= 2) & (categories < 4), remote, own_base + second_local)
    return jnp.stack([senders, receivers]).astype(jnp.int32)


def draw_edge_owned(key, part):
    subkeys = jax.random.split(jax.random.fold_in(key, 17), 2)
    counts = jax.random.randint(subkeys[0], (N_BLK,), EDGE_DEV * 5 // 8, EDGE_DEV + 1)
    fullest = jax.random.randint(subkeys[1], (), 0, N_BLK)
    counts = jnp.where(jnp.arange(N_BLK) == fullest, EDGE_DEV, counts)
    slots = jnp.arange(EDGE_DEV)[None, :] < counts[:, None]
    return slots.astype(jnp.int32).reshape(-1)


def pick_rows(subkey):
    return jax.random.permutation(subkey, NODE_DEV)[:HALO]


def draw_send_index(key, part):
    subkeys = jax.random.split(jax.random.fold_in(key, 23), N_BLK * FACES)
    picked = jax.vmap(pick_rows)(subkeys)
    return picked.reshape(N_BLK, FACES, HALO).astype(jnp.int32)


def steps_of(rng, extent, cuts, least, high):
    loudness, own = 1.0, jax.random.fold_in(rng, 6)
    for dim, parts in cuts:
        steps = jnp.exp(jax.random.uniform(jax.random.fold_in(own, dim), (parts,), jnp.float32, least / len(cuts), high / len(cuts)))
        loudness = loudness * jnp.repeat(steps, extent[dim] // parts).reshape([-1 if axis == dim else 1 for axis in range(len(extent))])
    return loudness


def noise(key, shape, scale, limit, cuts=(), kind=jnp.bfloat16):
    level = steps_of(key, shape, cuts, -0.22, 0.18) if cuts else 1.0
    values = jax.random.normal(key, shape, jnp.float32) * scale * level
    return jnp.minimum(jnp.maximum(values, -limit), limit).astype(kind)


def setup_inputs(seed: int = 0) -> dict:
    arg_keys = jax.random.split(jax.random.key(seed), 16)
    node_latent = draw_node_latent(jax.random.fold_in(arg_keys[15], 71), 0)
    edge_latent = noise(arg_keys[1], (EDGES, LATENT), 1.0, 6.0, ((0, 32),))
    edge_ends = draw_edge_ends(jax.random.fold_in(arg_keys[15], 71), 0)
    edge_owned = draw_edge_owned(jax.random.fold_in(arg_keys[15], 71), 0)
    send_index = draw_send_index(jax.random.fold_in(arg_keys[15], 71), 0)
    edge_w1 = noise(arg_keys[5], (LAYERS, 3 * LATENT, LATENT), (3 * LATENT) ** -0.5, 0.3125)
    edge_b1 = noise(arg_keys[6], (LAYERS, LATENT), 0.5, 3.0, (), jnp.float32)
    edge_w2 = noise(arg_keys[7], (LAYERS, LATENT, LATENT), LATENT ** -0.5, 0.5)
    edge_gain = jnp.clip(1.0 + 0.1 * jax.random.normal(arg_keys[8], (LAYERS, LATENT), jnp.float32), 0.5, 1.5)
    edge_shift = noise(arg_keys[9], (LAYERS, LATENT), 0.3, 2.0, (), jnp.float32)
    node_w1 = noise(arg_keys[10], (LAYERS, 2 * LATENT, LATENT), (2 * LATENT) ** -0.5, 0.375)
    node_b1 = noise(arg_keys[11], (LAYERS, LATENT), 0.5, 3.0, (), jnp.float32)
    node_w2 = noise(arg_keys[12], (LAYERS, LATENT, LATENT), LATENT ** -0.5, 0.5)
    node_gain = jnp.clip(1.0 + 0.1 * jax.random.normal(arg_keys[13], (LAYERS, LATENT), jnp.float32), 0.5, 1.5)
    node_shift = noise(arg_keys[14], (LAYERS, LATENT), 0.3, 2.0, (), jnp.float32)
    return {"node_latent": node_latent, "edge_latent": edge_latent, "edge_ends": edge_ends, "edge_owned": edge_owned, "send_index": send_index, "edge_w1": edge_w1, "edge_b1": edge_b1, "edge_w2": edge_w2, "edge_gain": edge_gain, "edge_shift": edge_shift, "node_w1": node_w1, "node_b1": node_b1, "node_w2": node_w2, "node_gain": node_gain, "node_shift": node_shift}


def row_norm(mixed):
    centre = mixed - lax.optimization_barrier(jnp.mean(mixed, axis=1, keepdims=True))
    spread = lax.optimization_barrier(jnp.mean(centre * centre, axis=1, keepdims=True))
    return centre * lax.rsqrt(spread + 1e-05)

def reference(node_latent, edge_latent, edge_ends, edge_owned, send_index, edge_w1, edge_b1, edge_w2, edge_gain, edge_shift, node_w1, node_b1, node_w2, node_gain, node_shift):
    offsets = jnp.array([1, -1, GX, -GX, GX * GY, -GX * GY], dtype=jnp.int32)
    blocks = jnp.arange(N_BLK, dtype=jnp.int32)
    source = jnp.mod(blocks[:, None] - offsets[None, :], N_BLK).astype(jnp.int32)
    face_ids = jnp.arange(FACES, dtype=jnp.int32)[None, :]
    halo_nodes = source[:, :, None] * NODE_DEV + send_index[source, face_ids]
    own_nodes = blocks[:, None] * NODE_DEV + jnp.arange(NODE_DEV, dtype=jnp.int32)[None, :]
    lookup = jnp.concatenate([own_nodes, halo_nodes.reshape(N_BLK, FACES * HALO)], axis=1).astype(jnp.int32)
    ends = edge_ends.reshape(2, N_BLK, EDGE_DEV)
    senders = jnp.take_along_axis(lookup, ends[0], axis=1)
    receivers = jnp.take_along_axis(lookup, ends[1], axis=1)
    owned = edge_owned.reshape(N_BLK, EDGE_DEV).astype(jnp.float32)
    latents = node_latent
    edge_state = edge_latent.reshape(N_BLK, EDGE_DEV, LATENT)
    for layer_id in range(LAYERS):

        def edge_block(totals, item, latents=latents, layer_id=layer_id):
            block_edges, block_send, block_recv, block_owned = item
            joined = jnp.concatenate([block_edges, latents[block_send], latents[block_recv]], axis=1)
            hidden = jax.nn.relu(jnp.dot(joined, edge_w1[layer_id], preferred_element_type=jnp.float32) + edge_b1[layer_id]).astype(jnp.bfloat16)
            mixed = jnp.dot(hidden, edge_w2[layer_id], preferred_element_type=jnp.float32)
            normed = edge_gain[layer_id] * row_norm(mixed) + edge_shift[layer_id]
            edges_new = (block_edges.astype(jnp.float32) + block_owned[:, None] * normed).astype(jnp.bfloat16)
            totals = totals.at[block_recv].add(block_owned[:, None] * edges_new.astype(jnp.float32))
            return (totals, edges_new)
        start = jnp.zeros((N_BLK * NODE_DEV, LATENT), jnp.float32)
        totals, edge_state = lax.scan(edge_block, start, (edge_state, senders, receivers, owned))
        aggregate = totals.astype(jnp.bfloat16)
        node_in = jnp.concatenate([latents, aggregate], axis=1)
        node_hidden = jax.nn.relu(jnp.dot(node_in, node_w1[layer_id], preferred_element_type=jnp.float32) + node_b1[layer_id]).astype(jnp.bfloat16)
        update = jnp.dot(node_hidden, node_w2[layer_id], preferred_element_type=jnp.float32)
        centre_mean = lax.optimization_barrier(jnp.mean(update, axis=0))
        deviation = update - centre_mean
        variance = lax.optimization_barrier(jnp.mean(deviation * deviation, axis=0))
        latents = (latents.astype(jnp.float32) + node_gain[layer_id] * deviation * lax.rsqrt(variance + 1e-05) + node_shift[layer_id]).astype(jnp.bfloat16)
    return (latents, edge_state.reshape(N_BLK * EDGE_DEV, LATENT))
```

```python
import functools

import jax
import jax.numpy as jnp
from jax import lax
from jax.experimental import pallas as pl
from jax.experimental.pallas import tpu as pltpu
from jax.sharding import PartitionSpec as P

LAYERS = 2
FACES = 6
GX = 4
GY = 4
TILE = 128
UNITS = 8
CHUNKS = 8
MESH = pl.DeviceIdType.MESH
VMEM = pltpu.VMEM
F32 = jnp.float32
BF16 = jnp.bfloat16
I32 = jnp.int32
I16 = jnp.int16


def dot(a, b):
    return jnp.dot(a, b, preferred_element_type=F32)


def dot_t(a, b):
    return lax.dot_general(a, b, (((1,), (1,)), ((), ())), preferred_element_type=F32)


def iota(shape, axis):
    return lax.broadcasted_iota(I32, shape, axis)


def hot_rows(row, rows):
    width = row.shape[1]
    wide = jnp.broadcast_to(row, (16, width)).astype(I16)
    wide = jnp.concatenate([wide] * (rows // 16), axis=0)
    return jnp.where(wide == iota((rows, width), 0).astype(I16), jnp.ones((), BF16), jnp.zeros((), BF16))


def column(row):
    return jnp.broadcast_to(row, (TILE, TILE)).T


def twice(block):
    return jnp.concatenate([block, block], axis=1)


def face_target(me, face, n, sign):
    step = jnp.where(face < 2, 1, jnp.where(face < 4, GX, GX * GY))
    step = jnp.where(face % 2 == 0, step, -step) * sign
    return lax.rem(me + step + n * GX * GY, n)


def mesh_kernel(n, h_ref, e_ref, ends_ref, owned_ref, send_ref, ew1_ref, eb1_ref, ew2_ref, egain_ref, eshift_ref,
                nw1_ref, nb1_ref, nw2_ref, ngain_ref, nshift_ref,
                hout_ref, eout_ref,
                ht, estage, et, hid, ptab, phalo, own_acc, halo_acc, upd, scol, w1e, w1sr, w2c, cols, nw1, nw2,
                stage, landed, hsend, returned, sums, mine, stats,
                esem, osem, lsend, lrecv, bsend, brecv, tsem, usem):
    me = lax.axis_index("blk")
    own_rows, width = h_ref.shape
    halo_rows = stage.shape[3]
    groups = own_rows // TILE
    barrier = pltpu.get_barrier_semaphore()

    @pl.loop(1, n)
    def _(j):
        pl.semaphore_signal(barrier, inc=1, device_id=(lax.rem(me + j, n),), device_id_type=MESH)

    edges_in = pltpu.make_async_copy(e_ref, estage, esem)
    edges_in.start()

    def latents_copy(layer, k):
        return pltpu.make_async_remote_copy(
            src_ref=stage.at[layer, k], dst_ref=landed.at[layer, k], send_sem=lsend.at[layer, k],
            recv_sem=lrecv.at[layer, k], device_id=(face_target(me, k, n, 1),), device_id_type=MESH)

    def sums_copy(layer, k):
        return pltpu.make_async_remote_copy(
            src_ref=hsend.at[layer, k], dst_ref=returned.at[layer, k], send_sem=bsend.at[layer, k],
            recv_sem=brecv.at[layer, k], device_id=(face_target(me, k, n, -1),), device_id_type=MESH)

    def stats_copy(layer, j):
        return pltpu.make_async_remote_copy(
            src_ref=mine.at[layer], dst_ref=stats.at[layer, me], send_sem=tsem.at[layer, j],
            recv_sem=usem.at[layer, j], device_id=(lax.rem(me + j, n),), device_id_type=MESH)

    def edges_out(q):
        at = pl.ds(2 * q, 2)
        return pltpu.make_async_copy(et.at[:, at], eout_ref.at[:, at], osem.at[q])

    for j in range(groups // 4):
        for i in range(j * 4, j * 4 + 4):
            ht[:, i * TILE:(i + 1) * TILE] = h_ref[i * TILE:(i + 1) * TILE, :].T
    for j in range(FACES * halo_rows // TILE):
        row = send_ref[0:1, j * TILE:(j + 1) * TILE]
        scol[j * TILE:(j + 1) * TILE, :] = column(row).astype(I16)

    def gather(layer, k0):
        totals = [None] * 2
        rows = [send_ref[0:1, pl.ds(pl.multiple_of((k0 + f) * halo_rows, TILE), halo_rows)] for f in range(2)]
        for b in range(own_rows // 256):
            for f in range(2):
                part = dot(ht[:, b * 256:(b + 1) * 256], hot_rows(rows[f] - b * 256, 256))
                totals[f] = part if totals[f] is None else totals[f] + part
        for f in range(2):
            stage[layer, pl.ds(k0 + f, 1)] = totals[f].astype(BF16)[None]
            latents_copy(layer, k0 + f).start()

    def load_edge_weights(layer):
        w1e[...] = ew1_ref[layer, 0:width, :].T
        w1sr[0:width, :] = ew1_ref[layer, width:2 * width, :].T
        w1sr[width:2 * width, :] = ew1_ref[layer, 2 * width:3 * width, :].T
        second = ew2_ref[layer].astype(F32).T
        second = second - jnp.mean(second, axis=0, keepdims=True)
        w2c[...] = second.astype(BF16)
        cols[0] = column(0.5 * eb1_ref[layer:layer + 1, :])
        cols[1] = column(egain_ref[layer:layer + 1, :])
        cols[2] = column(eshift_ref[layer:layer + 1, :])

    def load_node_weights(layer):
        nw1[...] = nw1_ref[layer].T
        nw2[...] = nw2_ref[layer].T
        cols[3] = column(nb1_ref[layer:layer + 1, :])

    def own_tables():
        chunk = 4 * TILE

        @pl.loop(0, own_rows // chunk // 2)
        def _(c):
            for half in range(2):
                first = pl.multiple_of((c * 2 + half) * chunk, chunk)
                both = dot(w1sr[...], ht[:, pl.ds(first, chunk)])
                both = (both + twice(twice(jnp.concatenate([cols[0], cols[0]], axis=0)))).astype(BF16)
                for j in range(4):
                    at = slice(j * TILE, (j + 1) * TILE)
                    ptab[pl.ds((c * 2 + half) * 4 + j, 1)] = jnp.concatenate(
                        [both[:width, at], both[width:, at]], axis=1)[None]
                    own_acc[pl.ds((c * 2 + half) * 4 + j, 1)] = jnp.zeros((1, TILE, TILE), F32)

    def ends_of(group, face):
        first = pl.multiple_of((group * FACES + face) * TILE, TILE)
        s = ends_ref[0:1, pl.ds(first, TILE)]
        r = ends_ref[1:2, pl.ds(first, TILE)]
        ok = owned_ref[0:1, pl.ds(first, TILE)] > 0
        return s, r, ok, r >= own_rows

    def both_tiles(pick, group, k0):
        return jnp.concatenate([pick(group, k0), pick(group, k0 + 1)], axis=1)

    def send_row(group, face):
        s, _, _, _ = ends_of(group, face)
        return jnp.where(s >= own_rows, -1, s - group * TILE)

    def receive_row(group, face):
        _, r, ok, r_halo = ends_of(group, face)
        return jnp.where(ok & ~r_halo, r - group * TILE, -1)

    def halo_row(group, face):
        s, r, ok, r_halo = ends_of(group, face)
        return jnp.where(ok, jnp.where(r_halo, r, s) - (own_rows + face * halo_rows), -1)

    def halo_flag(group, face):
        _, _, ok, r_halo = ends_of(group, face)
        return jnp.where(ok & r_halo, 1.0, 0.0)

    def halo_receive_row(group, face):
        _, r, ok, r_halo = ends_of(group, face)
        return jnp.where(ok & r_halo, r - (own_rows + face * halo_rows), -1)

    def both_groups(pick, pair, face):
        return jnp.concatenate([pick(pair * 2, face), pick(pair * 2 + 1, face)], axis=1)

    def gather_stage(layer, u, pair, k0):
        from_halo = [[None] * 2, [None] * 2]
        for f in range(2):
            both = dot(phalo[f], hot_rows(both_groups(halo_row, pair, k0 + f), halo_rows))
            for g in range(2):
                part = both[:, g * TILE:(g + 1) * TILE]
                flag = jnp.broadcast_to(halo_flag(pair * 2 + g, k0 + f), (width, TILE)) > 0.5
                from_halo[g][f] = jnp.where(flag, part[width:], part[:width])
        for g in range(2):
            group = pair * 2 + g
            old = []
            for f in range(2):
                if layer == 0:
                    first = pl.multiple_of((group * FACES + k0 + f) * TILE, TILE)
                    old.append(estage[pl.ds(first, TILE), :].T)
                    et[group, k0 + f] = old[f]
                else:
                    old.append(et[group, k0 + f])
            hots = jnp.concatenate([hot_rows(both_tiles(send_row, group, k0), TILE),
                                    hot_rows(both_tiles(receive_row, group, k0), TILE),
                                    jnp.concatenate(old, axis=1)], axis=0)
            before = dot(jnp.concatenate([ptab[group], w1e[...]], axis=1), hots)
            before = before + jnp.concatenate(from_halo[g], axis=1)
            hid[u, g] = jnp.maximum(before, 0.0).astype(BF16)

    def mix_stage(layer, u, pair, k0):
        for g in range(2):
            group = pair * 2 + g
            centre = dot(w2c[...], hid[u, g])
            spread = jnp.mean(centre * centre, axis=0, keepdims=True)
            ok = jnp.concatenate([owned_ref[0:1, pl.ds(pl.multiple_of((group * FACES + k0 + f) * TILE, TILE), TILE)]
                                  for f in range(2)], axis=1)
            keep = jnp.broadcast_to(ok, centre.shape) > 0
            normed = twice(cols[1]) * (centre * lax.rsqrt(spread + 1e-05)) + twice(cols[2])
            old = jnp.concatenate([et[group, k0], et[group, k0 + 1]], axis=1)
            new = (old.astype(F32) + jnp.where(keep, normed, 0.0)).astype(BF16)
            for f in range(2):
                et[group, k0 + f] = new[:, f * TILE:(f + 1) * TILE]

    def scatter_stage(pairs, k0):
        for pair in pairs:
            for g in range(2):
                group = pair * 2 + g
                new = jnp.concatenate([et[group, k0], et[group, k0 + 1]], axis=1)
                own_acc[group] += dot_t(new, hot_rows(both_tiles(receive_row, group, k0), TILE))
        for f in range(2):
            sent = jnp.concatenate([et[pair * 2 + g, k0 + f] for pair in pairs for g in range(2)], axis=1)
            hots = jnp.concatenate([hot_rows(both_groups(halo_receive_row, pair, k0 + f), halo_rows) for pair in pairs], axis=1)
            halo_acc[f] += dot_t(sent, hots)

    def edge_phase(layer, q):
        k0 = 2 * q
        for f in range(2):
            latents_copy(layer, k0 + f).wait_recv()
            half_bias = twice(jnp.concatenate([cols[0], cols[0]], axis=0))
            phalo[f] = (dot(w1sr[...], landed[layer, k0 + f]) + half_bias).astype(BF16)
        halo_acc[...] = jnp.zeros_like(halo_acc)
        steps = groups // 2 // UNITS

        def units(i):
            return [i * UNITS + u for u in range(UNITS)]

        def stage_one(i):
            for u, pair in enumerate(units(i)):
                gather_stage(layer, u, pair, k0)

        def stage_two(i):
            for u, pair in enumerate(units(i)):
                mix_stage(layer, u, pair, k0)

        def stage_three(i):
            scatter_stage(units(i), k0)

        @pl.loop(0, steps)
        def _(i):
            stage_one(i)
            stage_two(i)
            stage_three(i)

        for f in range(2):
            hsend[layer, pl.ds(k0 + f, 1)] = halo_acc[f].astype(BF16)[None]
            sums_copy(layer, k0 + f).start()
        if layer == LAYERS - 1:
            edges_out(q).start()

    def slots(layer, faces, base):
        lane = iota((halo_rows, TILE), 1)
        hots = []
        for j in range(2):
            goal = (lane + (base + j * TILE)).astype(I16)
            hots.append(jnp.concatenate(
                [jnp.where(scol[k * halo_rows:(k + 1) * halo_rows, :] == goal, jnp.ones((), BF16), jnp.zeros((), BF16))
                 for k in faces], axis=0))
        values = jnp.concatenate([returned[layer, k] for k in faces], axis=1)
        return dot(values, jnp.concatenate(hots, axis=1))

    def early_sums(layer, faces):
        for k in faces:
            sums_copy(layer, k).wait_recv()

        @pl.loop(0, own_rows // 256 // CHUNKS)
        def _(c):
            for i in range(CHUNKS):
                pair = c * CHUNKS + i
                extra = slots(layer, faces, pair * 256)
                own_acc[pair * 2] += extra[:, :TILE]
                own_acc[pair * 2 + 1] += extra[:, TILE:]

    def node_mlp(layer, faces):
        for k in faces:
            sums_copy(layer, k).wait_recv()
        sums[...] = jnp.zeros_like(sums)

        @pl.loop(0, own_rows // 256 // CHUNKS)
        def _(c):
            joined, hidden = [], []
            for i in range(CHUNKS):
                pair = c * CHUNKS + i
                own = jnp.concatenate([own_acc[pair * 2], own_acc[pair * 2 + 1]], axis=1)
                agg = (own + slots(layer, faces, pair * 256)).astype(BF16)
                at = pl.ds(pl.multiple_of(pair * 256, 256), 256)
                joined.append(jnp.concatenate([ht[:, at], agg], axis=0))
            for i in range(CHUNKS):
                hidden.append(jnp.maximum(dot(nw1[...], joined[i]) + twice(cols[3]), 0.0).astype(BF16))
            for i in range(CHUNKS):
                update = dot(nw2[...], hidden[i])
                upd[:, pl.ds(pl.multiple_of((c * CHUNKS + i) * 256, 256), 256)] = update
                square = update * update
                sums[0] += update[:, :TILE] + update[:, TILE:]
                sums[1] += square[:, :TILE] + square[:, TILE:]

        packed = jnp.concatenate([jnp.sum(sums[i].T, axis=0, keepdims=True) for i in range(2)], axis=0)
        mine[layer] = packed
        stats[layer, pl.ds(me, 1)] = packed[None]

        @pl.loop(1, n)
        def _(j):
            stats_copy(layer, j).start()

    def node_norm(layer, target):
        @pl.loop(1, n)
        def _(j):
            stats_copy(layer, j).wait()

        total = jnp.sum(stats[layer], axis=0)
        count = own_rows * n
        mean = total[0:1] / count
        variance = jnp.maximum(total[1:2] / count - mean * mean, 0.0)
        scale = ngain_ref[layer:layer + 1, :] * lax.rsqrt(variance + 1e-05)
        cols[4] = column(scale)
        cols[5] = column(nshift_ref[layer:layer + 1, :] - scale * mean)

        @pl.loop(0, own_rows // 512)
        def _(c):
            for half in range(2):
                at = pl.ds(pl.multiple_of((c * 2 + half) * 256, 256), 256)
                target[:, at] = (ht[:, at].astype(F32) + twice(cols[4]) * upd[:, at] + twice(cols[5])).astype(BF16)

    load_edge_weights(0)
    load_node_weights(0)
    pl.semaphore_wait(barrier, n - 1)
    for layer in range(LAYERS):
        @pl.loop(0, FACES // 2)
        def _(p):
            gather(layer, 2 * lax.rem(p + 1, FACES // 2))

        own_tables()
        if layer == 0:
            edges_in.wait()

        @pl.loop(0, FACES // 2)
        def _(p):
            edge_phase(layer, lax.rem(p + 1, FACES // 2))

        early_sums(layer, (2, 3, 4, 5))
        node_mlp(layer, (0, 1))
        if layer < LAYERS - 1:
            load_edge_weights(layer + 1)
            load_node_weights(layer + 1)
        node_norm(layer, hout_ref if layer == LAYERS - 1 else ht)

        @pl.loop(0, FACES)
        def _(k):
            latents_copy(layer, k).wait_send()
            sums_copy(layer, k).wait_send()

    @pl.loop(0, FACES // 2)
    def _(q):
        edges_out(q).wait()


def turn_kernel(ht_ref, et_ref, h_ref, e_ref):
    width = ht_ref.shape[0]
    for i in range(ht_ref.shape[1] // TILE):
        h_ref[i * TILE:(i + 1) * TILE, :] = ht_ref[:, i * TILE:(i + 1) * TILE].T
        for k in range(FACES):
            first = (i * FACES + k) * TILE
            e_ref[first:first + TILE, :] = et_ref[i, k].T


def per_device(n, node_latent, edge_latent, edge_ends, edge_owned, send_index, edge_w1, edge_b1, edge_w2,
               edge_gain, edge_shift, node_w1, node_b1, node_w2, node_gain, node_shift):
    own_rows, width = node_latent.shape
    slots = edge_latent.shape[0]
    halo_rows = send_index.shape[2]
    groups = own_rows // TILE
    vmem = pl.BlockSpec(memory_space=VMEM)
    anywhere = pl.BlockSpec(memory_space=pl.ANY)
    faces = (LAYERS, FACES, width, halo_rows)
    sems = pltpu.SemaphoreType.DMA((LAYERS, FACES))
    peers = pltpu.SemaphoreType.DMA((LAYERS, n))
    ht, et = pl.pallas_call(
        functools.partial(mesh_kernel, n),
        in_specs=[vmem, anywhere] + [vmem] * 13,
        out_specs=[vmem, anywhere],
        out_shape=[jax.ShapeDtypeStruct((width, own_rows), BF16),
                   jax.ShapeDtypeStruct((groups, FACES, width, TILE), BF16)],
        scratch_shapes=[
            VMEM((width, own_rows), BF16),
            VMEM((slots, width), BF16),
            VMEM((groups, FACES, width, TILE), BF16),
            VMEM((UNITS, 2, width, 2 * TILE), BF16),
            VMEM((groups, width, 2 * TILE), BF16),
            VMEM((2, 2 * width, halo_rows), BF16),
            VMEM((groups, width, TILE), F32),
            VMEM((2, width, halo_rows), F32),
            VMEM((width, own_rows), F32),
            VMEM((FACES * halo_rows, TILE), I16),
            VMEM((width, width), BF16),
            VMEM((2 * width, width), BF16),
            VMEM((width, width), BF16),
            VMEM((6, width, TILE), F32),
            VMEM((width, 2 * width), BF16),
            VMEM((width, width), BF16),
            VMEM(faces, BF16), VMEM(faces, BF16), VMEM(faces, BF16), VMEM(faces, BF16),
            VMEM((2, width, TILE), F32), VMEM((LAYERS, 2, width), F32), VMEM((LAYERS, n, 2, width), F32),
            pltpu.SemaphoreType.DMA, pltpu.SemaphoreType.DMA((FACES // 2,)),
            sems, sems, sems, sems, peers, peers,
        ],
        compiler_params=pltpu.CompilerParams(collective_id=0, has_side_effects=True),
    )(node_latent, edge_latent, edge_ends, edge_owned.reshape(1, slots), send_index.reshape(1, FACES * halo_rows),
      edge_w1, edge_b1, edge_w2, edge_gain, edge_shift, node_w1, node_b1, node_w2, node_gain, node_shift)
    per = 4 if groups % 4 == 0 else 1
    return pl.pallas_call(
        turn_kernel,
        grid=(groups // per,),
        in_specs=[pl.BlockSpec((width, per * TILE), lambda i: (0, i)),
                  pl.BlockSpec((per, FACES, width, TILE), lambda i: (i, 0, 0, 0))],
        out_specs=[pl.BlockSpec((per * TILE, width), lambda i: (i, 0)),
                   pl.BlockSpec((per * FACES * TILE, width), lambda i: (i, 0))],
        out_shape=[jax.ShapeDtypeStruct((own_rows, width), BF16),
                   jax.ShapeDtypeStruct((slots, width), BF16)],
        compiler_params=pltpu.CompilerParams(dimension_semantics=("arbitrary",)),
    )(ht, et)


def solution(mesh):
    row, rep = P("blk", None), P()
    return jax.shard_map(
        functools.partial(per_device, mesh.shape["blk"]),
        mesh=mesh,
        in_specs=(row, row, P(None, "blk"), P("blk"), P("blk", None, None)) + (rep,) * 10,
        out_specs=(row, row),
        check_vma=False,
    )
```

```python
import functools

import jax
import jax.numpy as jnp
from jax import lax
from jax.experimental import pallas as pl
from jax.experimental.pallas import tpu as pltpu
from jax.sharding import PartitionSpec as P

LAYERS = 2
FACES = 6
GX = 4
GY = 4
TILE = 128
UNITS = 16
LAG = 2
SPAN = 2
CHUNKS = 8
MESH = pl.DeviceIdType.MESH
VMEM = pltpu.VMEM
F32 = jnp.float32
BF16 = jnp.bfloat16
I32 = jnp.int32
I16 = jnp.int16


def dot(a, b):
    return jnp.dot(a, b, preferred_element_type=F32)


def dot_t(a, b):
    return lax.dot_general(a, b, (((1,), (1,)), ((), ())), preferred_element_type=F32)


def iota(shape, axis):
    return lax.broadcasted_iota(I32, shape, axis)


def hot_rows(row, rows):
    width = row.shape[1]
    wide = jnp.broadcast_to(row, (16, width)).astype(I16)
    wide = jnp.concatenate([wide] * (rows // 16), axis=0)
    return jnp.where(wide == iota((rows, width), 0).astype(I16), jnp.ones((), BF16), jnp.zeros((), BF16))


def column(row):
    return jnp.broadcast_to(row, (TILE, TILE)).T


def twice(block):
    return jnp.concatenate([block, block], axis=1)


def face_pair(phase):
    return lax.rem(2 * phase, FACES // 2)


def face_target(me, face, n, sign):
    step = jnp.where(face < 2, 1, jnp.where(face < 4, GX, GX * GY))
    step = jnp.where(face % 2 == 0, step, -step) * sign
    return lax.rem(me + step + n * GX * GY, n)


def mesh_kernel(n, h_in, e_ref, ends_in, owned_in, send_in, ew1_in, eb1_in, ew2_in, egain_in, eshift_in,
                nw1_in, nb1_in, nw2_in, ngain_in, nshift_in,
                hout_ref, et,
                h_ref, ends_ref, owned_ref, send_ref, ew1_ref, eb1_ref, ew2_ref, egain_ref, eshift_ref,
                nw1_ref, nb1_ref, nw2_ref, ngain_ref, nshift_ref,
                ht, ahead, estage, hid, ptab, phalo, own_acc, halo_acc, upd, scol, w1e, w1sr, w2c, cols, nw1, nw2,
                stage, landed, hsend, returned, sums, mine, stats,
                esem, isem, lsend, lrecv, bsend, brecv, tsem, usem):
    inputs = [(h_in, h_ref), (send_in, send_ref), (ew1_in, ew1_ref), (eb1_in, eb1_ref), (ew2_in, ew2_ref),
              (egain_in, egain_ref), (eshift_in, eshift_ref), (nw1_in, nw1_ref), (nb1_in, nb1_ref), (nw2_in, nw2_ref),
              (ngain_in, ngain_ref), (nshift_in, nshift_ref), (ends_in, ends_ref), (owned_in, owned_ref)]
    loads = [pltpu.make_async_copy(source, target, isem.at[i]) for i, (source, target) in enumerate(inputs)]
    for load in loads:
        load.start()
    edges_in = pltpu.make_async_copy(e_ref, estage, esem)
    edges_in.start()
    me = lax.axis_index("blk")
    own_rows, width = h_ref.shape
    halo_rows = stage.shape[3]
    groups = own_rows // TILE
    barrier = pltpu.get_barrier_semaphore()

    @pl.loop(1, n)
    def _(j):
        pl.semaphore_signal(barrier, inc=1, device_id=(lax.rem(me + j, n),), device_id_type=MESH)

    def latents_copy(layer, k):
        return pltpu.make_async_remote_copy(
            src_ref=stage.at[layer, k], dst_ref=landed.at[layer, k], send_sem=lsend.at[layer, k],
            recv_sem=lrecv.at[layer, k], device_id=(face_target(me, k, n, 1),), device_id_type=MESH)

    def sums_copy(layer, k):
        return pltpu.make_async_remote_copy(
            src_ref=hsend.at[layer, k], dst_ref=returned.at[layer, k], send_sem=bsend.at[layer, k],
            recv_sem=brecv.at[layer, k], device_id=(face_target(me, k, n, -1),), device_id_type=MESH)

    def stats_copy(layer, j):
        return pltpu.make_async_remote_copy(
            src_ref=mine.at[layer], dst_ref=stats.at[layer, me], send_sem=tsem.at[layer, j],
            recv_sem=usem.at[layer, j], device_id=(lax.rem(me + j, n),), device_id_type=MESH)

    loads[0].wait()
    for i in range(groups):
        ht[0:width, i * TILE:(i + 1) * TILE] = h_ref[i * TILE:(i + 1) * TILE, :].T
    for load in loads[1:]:
        load.wait()
    for j in range(FACES * halo_rows // TILE):
        row = send_ref[0:1, j * TILE:(j + 1) * TILE]
        scol[j * TILE:(j + 1) * TILE, :] = column(row).astype(I16)

    def gather(k0, rows):
        totals = [None] * 2
        picks = [send_ref[0:1, pl.ds(pl.multiple_of((k0 + f) * halo_rows, TILE), halo_rows)] for f in range(2)]
        for b in range(own_rows // 256):
            for f in range(2):
                part = dot(ht[0:rows, b * 256:(b + 1) * 256], hot_rows(picks[f] - b * 256, 256))
                totals[f] = part if totals[f] is None else totals[f] + part
        return totals

    def send_first():
        for phase in range(FACES // 2):
            k0 = 2 * (2 * phase % (FACES // 2))
            totals = gather(k0, width)
            if phase == 0:
                pl.semaphore_wait(barrier, n - 1)
            for f in range(2):
                stage[0, k0 + f] = totals[f].astype(BF16)
                latents_copy(0, k0 + f).start()

    def gather_ahead():
        @pl.loop(0, FACES // 2)
        def _(q):
            totals = gather(2 * q, 2 * width)
            for f in range(2):
                ahead[2 * q + f] = totals[f]

    def send_next(layer):
        @pl.loop(0, FACES // 2)
        def _(p):
            k0 = 2 * face_pair(p)
            for f in range(2):
                new = ahead[k0 + f, 0:width] + twice(cols[4]) * ahead[k0 + f, width:2 * width] + twice(cols[5])
                stage[layer, pl.ds(k0 + f, 1)] = new.astype(BF16)[None]
                latents_copy(layer, k0 + f).start()

    def turn_edges():
        @pl.loop(0, groups // 2)
        def _(i):
            turned = [et[i * 2 + g, k].T for g in range(2) for k in range(FACES)]
            for g in range(2):
                for k in range(FACES):
                    et[i * 2 + g, k] = turned[g * FACES + k]

    def load_edge_weights(layer):
        w1e[...] = ew1_ref[layer, 0:width, :].T
        w1sr[0:width, :] = ew1_ref[layer, width:2 * width, :].T
        w1sr[width:2 * width, :] = ew1_ref[layer, 2 * width:3 * width, :].T
        second = ew2_ref[layer].astype(F32).T
        second = second - jnp.mean(second, axis=0, keepdims=True)
        w2c[...] = second.astype(BF16)
        cols[0] = column(0.5 * eb1_ref[layer:layer + 1, :])
        cols[1] = column(egain_ref[layer:layer + 1, :])
        cols[2] = column(eshift_ref[layer:layer + 1, :])

    def load_node_weights(layer):
        nw1[...] = nw1_ref[layer].T
        nw2[...] = nw2_ref[layer].T
        cols[3] = column(nb1_ref[layer:layer + 1, :])

    def own_tables():
        chunk = 4 * TILE

        @pl.loop(0, own_rows // chunk // 2)
        def _(c):
            for half in range(2):
                first = pl.multiple_of((c * 2 + half) * chunk, chunk)
                both = dot(w1sr[...], ht[0:width, pl.ds(first, chunk)])
                both = (both + twice(twice(jnp.concatenate([cols[0], cols[0]], axis=0)))).astype(BF16)
                for j in range(4):
                    at = slice(j * TILE, (j + 1) * TILE)
                    ptab[pl.ds((c * 2 + half) * 4 + j, 1)] = jnp.concatenate(
                        [both[:width, at], both[width:, at]], axis=1)[None]
                    own_acc[pl.ds((c * 2 + half) * 4 + j, 1)] = jnp.zeros((1, TILE, TILE), F32)

    def ends_of(group, face):
        first = pl.multiple_of((group * FACES + face) * TILE, TILE)
        s = ends_ref[0:1, pl.ds(first, TILE)]
        r = ends_ref[1:2, pl.ds(first, TILE)]
        ok = owned_ref[0:1, pl.ds(first, TILE)] > 0
        return s, r, ok, r >= own_rows

    def both_tiles(pick, group, k0):
        return jnp.concatenate([pick(group, k0), pick(group, k0 + 1)], axis=1)

    def send_row(group, face):
        s, _, _, _ = ends_of(group, face)
        return jnp.where(s >= own_rows, -1, s - group * TILE)

    def receive_row(group, face):
        _, r, ok, r_halo = ends_of(group, face)
        return jnp.where(ok & ~r_halo, r - group * TILE, -1)

    def halo_row(group, face):
        s, r, ok, r_halo = ends_of(group, face)
        return jnp.where(ok, jnp.where(r_halo, r, s) - (own_rows + face * halo_rows), -1)

    def halo_flag(group, face):
        _, _, ok, r_halo = ends_of(group, face)
        return jnp.where(ok & r_halo, 1.0, 0.0)

    def halo_receive_row(group, face):
        _, r, ok, r_halo = ends_of(group, face)
        return jnp.where(ok & r_halo, r - (own_rows + face * halo_rows), -1)

    def both_groups(pick, pair, face):
        return jnp.concatenate([pick(pair * 2, face), pick(pair * 2 + 1, face)], axis=1)

    def gather_stage(layer, u, pair, k0):
        from_halo = [[None] * 2, [None] * 2]
        for f in range(2):
            both = dot(phalo[f], hot_rows(both_groups(halo_row, pair, k0 + f), halo_rows))
            for g in range(2):
                part = both[:, g * TILE:(g + 1) * TILE]
                flag = jnp.broadcast_to(halo_flag(pair * 2 + g, k0 + f), (width, TILE)) > 0.5
                from_halo[g][f] = jnp.where(flag, part[width:], part[:width])
        for g in range(2):
            group = pair * 2 + g
            old = []
            for f in range(2):
                if layer == 0:
                    first = pl.multiple_of((group * FACES + k0 + f) * TILE, TILE)
                    old.append(estage[pl.ds(first, TILE), :].T)
                    et[group, k0 + f] = old[f]
                else:
                    old.append(et[group, k0 + f])
            hots = jnp.concatenate([hot_rows(both_tiles(send_row, group, k0), TILE),
                                    hot_rows(both_tiles(receive_row, group, k0), TILE),
                                    jnp.concatenate(old, axis=1)], axis=0)
            before = dot(jnp.concatenate([ptab[group], w1e[...]], axis=1), hots)
            before = before + jnp.concatenate(from_halo[g], axis=1)
            hid[u, g] = jnp.maximum(before, 0.0).astype(BF16)

    def mix_stage(layer, u, pair, k0):
        for g in range(2):
            group = pair * 2 + g
            centre = dot(w2c[...], hid[u, g])
            spread = jnp.mean(centre * centre, axis=0, keepdims=True)
            ok = jnp.concatenate([owned_ref[0:1, pl.ds(pl.multiple_of((group * FACES + k0 + f) * TILE, TILE), TILE)]
                                  for f in range(2)], axis=1)
            keep = jnp.broadcast_to(ok, centre.shape) > 0
            normed = twice(cols[1]) * (centre * lax.rsqrt(spread + 1e-05)) + twice(cols[2])
            old = jnp.concatenate([et[group, k0], et[group, k0 + 1]], axis=1)
            new = (old.astype(F32) + jnp.where(keep, normed, 0.0)).astype(BF16)
            for f in range(2):
                et[group, k0 + f] = new[:, f * TILE:(f + 1) * TILE]

    def scatter_stage(pairs, k0):
        for pair in pairs:
            for g in range(2):
                group = pair * 2 + g
                new = jnp.concatenate([et[group, k0], et[group, k0 + 1]], axis=1)
                own_acc[group] += dot_t(new, hot_rows(both_tiles(receive_row, group, k0), TILE))
        for f in range(2):
            sent = jnp.concatenate([et[pair * 2 + g, k0 + f] for pair in pairs for g in range(2)], axis=1)
            hots = jnp.concatenate([hot_rows(both_groups(halo_receive_row, pair, k0 + f), halo_rows) for pair in pairs], axis=1)
            halo_acc[f] += dot_t(sent, hots)

    def edge_phase(layer, q):
        k0 = 2 * q
        for f in range(2):
            latents_copy(layer, k0 + f).wait_recv()
            half_bias = twice(jnp.concatenate([cols[0], cols[0]], axis=0))
            phalo[f] = (dot(w1sr[...], landed[layer, k0 + f]) + half_bias).astype(BF16)
        halo_acc[...] = jnp.zeros_like(halo_acc)

        @pl.loop(0, groups // 2 // UNITS)
        def _(i):
            for slot in range(UNITS + 2 * LAG + SPAN - 1):
                if slot < UNITS:
                    gather_stage(layer, slot, i * UNITS + slot, k0)
                if 0 <= slot - LAG < UNITS:
                    mix_stage(layer, slot - LAG, i * UNITS + slot - LAG, k0)
                done = slot - 2 * LAG + 1
                if 0 < done <= UNITS and done % SPAN == 0:
                    scatter_stage([i * UNITS + u for u in range(done - SPAN, done)], k0)

        for f in range(2):
            hsend[layer, pl.ds(k0 + f, 1)] = halo_acc[f].astype(BF16)[None]
            sums_copy(layer, k0 + f).start()

    def slots(layer, faces, base):
        lane = iota((halo_rows, TILE), 1)
        hots = []
        for j in range(2):
            goal = (lane + (base + j * TILE)).astype(I16)
            hots.append(jnp.concatenate(
                [jnp.where(scol[k * halo_rows:(k + 1) * halo_rows, :] == goal, jnp.ones((), BF16), jnp.zeros((), BF16))
                 for k in faces], axis=0))
        values = jnp.concatenate([returned[layer, k] for k in faces], axis=1)
        return dot(values, jnp.concatenate(hots, axis=1))

    def early_sums(layer, faces):
        for k in faces:
            sums_copy(layer, k).wait_recv()

        @pl.loop(0, own_rows // 256 // CHUNKS)
        def _(c):
            for i in range(CHUNKS):
                pair = c * CHUNKS + i
                extra = slots(layer, faces, pair * 256)
                own_acc[pair * 2] += extra[:, :TILE]
                own_acc[pair * 2 + 1] += extra[:, TILE:]

    def node_mlp(layer, faces):
        for k in faces:
            sums_copy(layer, k).wait_recv()
        sums[...] = jnp.zeros_like(sums)

        @pl.loop(0, own_rows // 256 // CHUNKS)
        def _(c):
            joined, hidden = [], []
            for i in range(CHUNKS):
                pair = c * CHUNKS + i
                own = jnp.concatenate([own_acc[pair * 2], own_acc[pair * 2 + 1]], axis=1)
                agg = (own + slots(layer, faces, pair * 256)).astype(BF16)
                at = pl.ds(pl.multiple_of(pair * 256, 256), 256)
                joined.append(jnp.concatenate([ht[0:width, at], agg], axis=0))
            for i in range(CHUNKS):
                hidden.append(jnp.maximum(dot(nw1[...], joined[i]) + twice(cols[3]), 0.0).astype(BF16))
            for i in range(CHUNKS):
                update = dot(nw2[...], hidden[i])
                at = pl.ds(pl.multiple_of((c * CHUNKS + i) * 256, 256), 256)
                upd[:, at] = update
                if layer < LAYERS - 1:
                    ht[width:2 * width, at] = update.astype(BF16)
                square = update * update
                sums[0] += update[:, :TILE] + update[:, TILE:]
                sums[1] += square[:, :TILE] + square[:, TILE:]

        packed = jnp.concatenate([jnp.sum(sums[i].T, axis=0, keepdims=True) for i in range(2)], axis=0)
        mine[layer] = packed
        stats[layer, pl.ds(me, 1)] = packed[None]

        @pl.loop(1, n)
        def _(j):
            stats_copy(layer, j).start()

    def node_norm(layer):
        last = layer == LAYERS - 1
        if last:
            turn_edges()
        else:
            gather_ahead()

        @pl.loop(1, n)
        def _(j):
            stats_copy(layer, j).wait()

        total = jnp.sum(stats[layer], axis=0)
        count = own_rows * n
        mean = total[0:1] / count
        variance = jnp.maximum(total[1:2] / count - mean * mean, 0.0)
        scale = ngain_ref[layer:layer + 1, :] * lax.rsqrt(variance + 1e-05)
        cols[4] = column(scale)
        cols[5] = column(nshift_ref[layer:layer + 1, :] - scale * mean)
        if not last:
            send_next(layer + 1)

        @pl.loop(0, own_rows // 512)
        def _(c):
            for half in range(2):
                at = pl.ds(pl.multiple_of((c * 2 + half) * 256, 256), 256)
                new = (ht[0:width, at].astype(F32) + twice(cols[4]) * upd[:, at] + twice(cols[5])).astype(BF16)
                if last:
                    hout_ref[at, :] = new.T
                else:
                    ht[0:width, at] = new

    load_edge_weights(0)
    load_node_weights(0)
    send_first()
    for layer in range(LAYERS):
        own_tables()
        if layer == 0:
            edges_in.wait()

        @pl.loop(0, FACES // 2)
        def _(p):
            edge_phase(layer, face_pair(p))

        early_sums(layer, (0, 1))
        early_sums(layer, (4, 5))
        node_mlp(layer, (2, 3))
        if layer < LAYERS - 1:
            load_edge_weights(layer + 1)
            load_node_weights(layer + 1)
        node_norm(layer)

        @pl.loop(0, FACES)
        def _(k):
            latents_copy(layer, k).wait_send()
            sums_copy(layer, k).wait_send()


def place_kernel(h_in, e_in, h_ref, e_ref, sems):
    parts = sems.shape[0] - 1
    rows = e_in.shape[0] // parts
    copies = [pltpu.make_async_copy(e_in.at[pl.ds(i * rows, rows)], e_ref.at[pl.ds(i * rows, rows)], sems.at[i])
              for i in range(parts)]
    copies.append(pltpu.make_async_copy(h_in, h_ref, sems.at[parts]))
    for copy in copies:
        copy.start()
    for copy in copies:
        copy.wait()


def per_device(n, node_latent, edge_latent, edge_ends, edge_owned, send_index, edge_w1, edge_b1, edge_w2,
               edge_gain, edge_shift, node_w1, node_b1, node_w2, node_gain, node_shift):
    own_rows, width = node_latent.shape
    slots = edge_latent.shape[0]
    halo_rows = send_index.shape[2]
    groups = own_rows // TILE
    vmem = pl.BlockSpec(memory_space=VMEM)
    faces = (LAYERS, FACES, width, halo_rows)
    sems = pltpu.SemaphoreType.DMA((LAYERS, FACES))
    peers = pltpu.SemaphoreType.DMA((LAYERS, n))
    inputs = (node_latent, edge_latent, edge_ends, edge_owned.reshape(1, slots), send_index.reshape(1, FACES * halo_rows),
              edge_w1, edge_b1, edge_w2, edge_gain, edge_shift, node_w1, node_b1, node_w2, node_gain, node_shift)
    inputs = [pltpu.with_memory_space_constraint(a, pltpu.HBM) for a in inputs]
    nodes, edges = pl.pallas_call(
        functools.partial(mesh_kernel, n),
        in_specs=[pl.BlockSpec(memory_space=pltpu.HBM)] * len(inputs),
        out_specs=[vmem, vmem],
        out_shape=[jax.ShapeDtypeStruct((own_rows, width), BF16),
                   jax.ShapeDtypeStruct((groups, FACES, width, TILE), BF16)],
        scratch_shapes=[VMEM(a.shape, a.dtype) for i, a in enumerate(inputs) if i != 1] + [
            VMEM((2 * width, own_rows), BF16), VMEM((FACES, 2 * width, halo_rows), F32),
            VMEM((slots, width), BF16),
            VMEM((UNITS, 2, width, 2 * TILE), BF16),
            VMEM((groups, width, 2 * TILE), BF16),
            VMEM((2, 2 * width, halo_rows), BF16),
            VMEM((groups, width, TILE), F32),
            VMEM((2, width, halo_rows), F32),
            VMEM((width, own_rows), F32),
            VMEM((FACES * halo_rows, TILE), I16),
            VMEM((width, width), BF16),
            VMEM((2 * width, width), BF16),
            VMEM((width, width), BF16),
            VMEM((6, width, TILE), F32),
            VMEM((width, 2 * width), BF16),
            VMEM((width, width), BF16),
            VMEM(faces, BF16), VMEM(faces, BF16), VMEM(faces, BF16), VMEM(faces, BF16),
            VMEM((2, width, TILE), F32), VMEM((LAYERS, 2, width), F32), VMEM((LAYERS, n, 2, width), F32),
            pltpu.SemaphoreType.DMA, pltpu.SemaphoreType.DMA((len(inputs) - 1,)),
            sems, sems, sems, sems, peers, peers,
        ],
        compiler_params=pltpu.CompilerParams(collective_id=0, has_side_effects=True, vmem_limit_bytes=44 * 2 ** 20),
    )(*inputs)
    results = [pltpu.with_memory_space_constraint(a, pltpu.VMEM) for a in (nodes, edges.reshape(slots, width))]
    parts = 6
    return pl.pallas_call(
        place_kernel,
        in_specs=[vmem, vmem],
        out_specs=[pl.BlockSpec(memory_space=pltpu.HBM)] * 2,
        out_shape=[jax.ShapeDtypeStruct((own_rows, width), BF16), jax.ShapeDtypeStruct((slots, width), BF16)],
        scratch_shapes=[pltpu.SemaphoreType.DMA((parts + 1,))],
        compiler_params=pltpu.CompilerParams(vmem_limit_bytes=4 * 2 ** 20),
    )(*results)


def solution(mesh):
    row, rep = P("blk", None), P()
    return jax.shard_map(
        functools.partial(per_device, mesh.shape["blk"]),
        mesh=mesh,
        in_specs=(row, row, P(None, "blk"), P("blk"), P("blk", None, None)) + (rep,) * 10,
        out_specs=(row, row),
        check_vma=False,
    )
```

```python
import functools

import jax
import jax.numpy as jnp
from jax import lax
from jax.experimental import pallas as pl
from jax.experimental.pallas import tpu as pltpu
from jax.sharding import PartitionSpec as P

LAYERS = 2
FACES = 6
GX = 4
GY = 4
TILE = 128
UNITS = 16
LAG = 1
SPAN = 1
CHUNKS = 8
MESH = pl.DeviceIdType.MESH
VMEM = pltpu.VMEM
F32 = jnp.float32
BF16 = jnp.bfloat16
I32 = jnp.int32
I16 = jnp.int16


def dot(a, b):
    return jnp.dot(a, b, preferred_element_type=F32)


def dot_t(a, b):
    return lax.dot_general(a, b, (((1,), (1,)), ((), ())), preferred_element_type=F32)


def iota(shape, axis):
    return lax.broadcasted_iota(I32, shape, axis)


def hot_rows(row, rows):
    width = row.shape[1]
    wide = jnp.broadcast_to(row, (16, width)).astype(I16)
    wide = jnp.concatenate([wide] * (rows // 16), axis=0)
    return jnp.where(wide == iota((rows, width), 0).astype(I16), jnp.ones((), BF16), jnp.zeros((), BF16))


def column(row):
    return jnp.broadcast_to(row, (TILE, TILE)).T


def twice(block):
    return jnp.concatenate([block, block], axis=1)


def face_pair(phase):
    return lax.rem(2 * phase, FACES // 2)


def face_target(me, face, n, sign):
    step = jnp.where(face < 2, 1, jnp.where(face < 4, GX, GX * GY))
    step = jnp.where(face % 2 == 0, step, -step) * sign
    return lax.rem(me + step + n * GX * GY, n)


def mesh_kernel(n, h_in, e_ref, ends_in, owned_in, send_in, ew1_in, eb1_in, ew2_in, egain_in, eshift_in,
                nw1_in, nb1_in, nw2_in, ngain_in, nshift_in,
                hout_ref, et,
                h_ref, ends_ref, owned_ref, send_ref, ew1_ref, eb1_ref, ew2_ref, egain_ref, eshift_ref,
                nw1_ref, nb1_ref, nw2_ref, ngain_ref, nshift_ref,
                ht, soon, ahead, estage, hid, ptab, phalo, own_acc, halo_acc, upd, scol, w1e, w1sr, w2c, cols, nw1, nw2,
                stage, landed, hsend, returned, sums, mine, stats,
                esem, isem, lsend, lrecv, bsend, brecv, tsem, usem):
    inputs = [(h_in, h_ref), (send_in, send_ref), (ew1_in, ew1_ref), (eb1_in, eb1_ref), (ew2_in, ew2_ref),
              (egain_in, egain_ref), (eshift_in, eshift_ref), (nw1_in, nw1_ref), (nb1_in, nb1_ref), (nw2_in, nw2_ref),
              (ngain_in, ngain_ref), (nshift_in, nshift_ref), (ends_in, ends_ref), (owned_in, owned_ref)]
    loads = [pltpu.make_async_copy(source, target, isem.at[i]) for i, (source, target) in enumerate(inputs)]
    for load in loads:
        load.start()
    edges_in = pltpu.make_async_copy(e_ref, estage, esem)
    edges_in.start()
    me = lax.axis_index("blk")
    own_rows, width = h_ref.shape
    halo_rows = stage.shape[3]
    groups = own_rows // TILE
    barrier = pltpu.get_barrier_semaphore()

    @pl.loop(1, n)
    def _(j):
        pl.semaphore_signal(barrier, inc=1, device_id=(lax.rem(me + j, n),), device_id_type=MESH)

    def latents_copy(layer, k):
        return pltpu.make_async_remote_copy(
            src_ref=stage.at[layer, k], dst_ref=landed.at[layer, k], send_sem=lsend.at[layer, k],
            recv_sem=lrecv.at[layer, k], device_id=(face_target(me, k, n, 1),), device_id_type=MESH)

    def sums_copy(layer, k):
        return pltpu.make_async_remote_copy(
            src_ref=hsend.at[layer, k], dst_ref=returned.at[layer, k], send_sem=bsend.at[layer, k],
            recv_sem=brecv.at[layer, k], device_id=(face_target(me, k, n, -1),), device_id_type=MESH)

    def stats_copy(layer, j):
        return pltpu.make_async_remote_copy(
            src_ref=mine.at[layer], dst_ref=stats.at[layer, me], send_sem=tsem.at[layer, j],
            recv_sem=usem.at[layer, j], device_id=(lax.rem(me + j, n),), device_id_type=MESH)

    loads[0].wait()
    for i in range(groups):
        ht[:, i * TILE:(i + 1) * TILE] = h_ref[i * TILE:(i + 1) * TILE, :].T
    for load in loads[1:]:
        load.wait()
    for j in range(FACES * halo_rows // TILE):
        row = send_ref[0:1, j * TILE:(j + 1) * TILE]
        scol[j * TILE:(j + 1) * TILE, :] = column(row)

    def gather(k0, source):
        totals = [None] * 2
        picks = [send_ref[0:1, pl.ds(pl.multiple_of((k0 + f) * halo_rows, TILE), halo_rows)] for f in range(2)]
        for b in range(own_rows // 256):
            for f in range(2):
                part = dot(source[:, b * 256:(b + 1) * 256], hot_rows(picks[f] - b * 256, 256))
                totals[f] = part if totals[f] is None else totals[f] + part
        return totals

    def send_first():
        for phase in range(FACES // 2):
            k0 = 2 * (2 * phase % (FACES // 2))
            totals = gather(k0, ht)
            if phase == 0:
                pl.semaphore_wait(barrier, n - 1)
            for f in range(2):
                stage[0, k0 + f] = totals[f].astype(BF16)
                latents_copy(0, k0 + f).start()

    def gather_ahead():
        @pl.loop(0, FACES // 2)
        def _(q):
            totals = gather(2 * q, soon)
            for f in range(2):
                ahead[2 * q + f] = totals[f]

    def send_next(layer):
        @pl.loop(0, FACES // 2)
        def _(p):
            k0 = 2 * face_pair(p)
            for f in range(2):
                old = stage[layer - 1, k0 + f].astype(F32)
                new = old + twice(cols[4]) * ahead[k0 + f] + twice(cols[5])
                stage[layer, pl.ds(k0 + f, 1)] = new.astype(BF16)[None]
                latents_copy(layer, k0 + f).start()

    def turn_edges():
        @pl.loop(0, groups // 2)
        def _(i):
            turned = [et[i * 2 + g, k].T for g in range(2) for k in range(FACES)]
            for g in range(2):
                for k in range(FACES):
                    et[i * 2 + g, k] = turned[g * FACES + k]

    def load_edge_weights(layer):
        w1e[...] = ew1_ref[layer, 0:width, :].T
        w1sr[0:width, :] = ew1_ref[layer, width:2 * width, :].T
        w1sr[width:2 * width, :] = ew1_ref[layer, 2 * width:3 * width, :].T
        second = ew2_ref[layer].astype(F32).T
        second = second - jnp.mean(second, axis=0, keepdims=True)
        w2c[...] = second.astype(BF16)
        cols[0] = column(0.5 * eb1_ref[layer:layer + 1, :])
        cols[1] = column(egain_ref[layer:layer + 1, :])
        cols[2] = column(eshift_ref[layer:layer + 1, :])

    def load_node_weights(layer):
        nw1[...] = nw1_ref[layer].T
        nw2[...] = nw2_ref[layer].T
        cols[3] = column(nb1_ref[layer:layer + 1, :])

    def own_tables():
        chunk = 4 * TILE

        @pl.loop(0, own_rows // chunk // 2)
        def _(c):
            for half in range(2):
                first = pl.multiple_of((c * 2 + half) * chunk, chunk)
                both = dot(w1sr[...], ht[:, pl.ds(first, chunk)])
                both = (both + twice(twice(jnp.concatenate([cols[0], cols[0]], axis=0)))).astype(BF16)
                for j in range(4):
                    at = slice(j * TILE, (j + 1) * TILE)
                    ptab[pl.ds((c * 2 + half) * 4 + j, 1)] = jnp.concatenate(
                        [both[:width, at], both[width:, at]], axis=1)[None]
                    own_acc[pl.ds((c * 2 + half) * 4 + j, 1)] = jnp.zeros((1, TILE, TILE), F32)

    def ends_of(group, face):
        first = pl.multiple_of((group * FACES + face) * TILE, TILE)
        s = ends_ref[0:1, pl.ds(first, TILE)]
        r = ends_ref[1:2, pl.ds(first, TILE)]
        ok = owned_ref[0:1, pl.ds(first, TILE)] > 0
        return s, r, ok, r >= own_rows

    def both_tiles(pick, group, k0):
        return jnp.concatenate([pick(group, k0), pick(group, k0 + 1)], axis=1)

    def send_row(group, face):
        s, _, _, _ = ends_of(group, face)
        return jnp.where(s >= own_rows, -1, s - group * TILE)

    def receive_row(group, face):
        _, r, ok, r_halo = ends_of(group, face)
        return jnp.where(ok & ~r_halo, r - group * TILE, -1)

    def halo_row(group, face):
        s, r, ok, r_halo = ends_of(group, face)
        return jnp.where(ok, jnp.where(r_halo, r, s) - (own_rows + face * halo_rows), -1)

    def halo_flag(group, face):
        _, _, ok, r_halo = ends_of(group, face)
        return jnp.where(ok & r_halo, 1.0, 0.0)

    def halo_receive_row(group, face):
        _, r, ok, r_halo = ends_of(group, face)
        return jnp.where(ok & r_halo, r - (own_rows + face * halo_rows), -1)

    def both_groups(pick, pair, face):
        return jnp.concatenate([pick(pair * 2, face), pick(pair * 2 + 1, face)], axis=1)

    def gather_stage(layer, u, pair, k0):
        own = []
        for g in range(2):
            group = pair * 2 + g
            old = []
            for f in range(2):
                if layer == 0:
                    first = pl.multiple_of((group * FACES + k0 + f) * TILE, TILE)
                    old.append(estage[pl.ds(first, TILE), :].T)
                    et[group, k0 + f] = old[f]
                else:
                    old.append(et[group, k0 + f])
            hots = jnp.concatenate([hot_rows(both_tiles(send_row, group, k0), TILE),
                                    hot_rows(both_tiles(receive_row, group, k0), TILE),
                                    jnp.concatenate(old, axis=1)], axis=0)
            before = dot(jnp.concatenate([ptab[group], w1e[...]], axis=1), hots)
            own.append(before)
        from_halo = [[None] * 2, [None] * 2]
        for f in range(2):
            both = dot(phalo[f], hot_rows(both_groups(halo_row, pair, k0 + f), halo_rows))
            for g in range(2):
                part = both[:, g * TILE:(g + 1) * TILE]
                flag = jnp.broadcast_to(halo_flag(pair * 2 + g, k0 + f), (width, TILE)) > 0.5
                from_halo[g][f] = jnp.where(flag, part[width:], part[:width])
        for g in range(2):
            before = own[g] + jnp.concatenate(from_halo[g], axis=1)
            hid[u, g] = jnp.maximum(before, 0.0).astype(BF16)

    def mix_stage(layer, u, pair, k0):
        for g in range(2):
            group = pair * 2 + g
            centre = dot(w2c[...], hid[u, g])
            spread = jnp.mean(centre * centre, axis=0, keepdims=True)
            ok = jnp.concatenate([owned_ref[0:1, pl.ds(pl.multiple_of((group * FACES + k0 + f) * TILE, TILE), TILE)]
                                  for f in range(2)], axis=1)
            keep = jnp.broadcast_to(ok, centre.shape) > 0
            normed = twice(cols[1]) * (centre * lax.rsqrt(spread + 1e-05)) + twice(cols[2])
            old = jnp.concatenate([et[group, k0], et[group, k0 + 1]], axis=1)
            new = (old.astype(F32) + jnp.where(keep, normed, 0.0)).astype(BF16)
            for f in range(2):
                et[group, k0 + f] = new[:, f * TILE:(f + 1) * TILE]

    def scatter_stage(pairs, k0):
        for pair in pairs:
            for g in range(2):
                group = pair * 2 + g
                new = jnp.concatenate([et[group, k0], et[group, k0 + 1]], axis=1)
                own_acc[group] += dot_t(new, hot_rows(both_tiles(receive_row, group, k0), TILE))
        for f in range(2):
            sent = jnp.concatenate([et[pair * 2 + g, k0 + f] for pair in pairs for g in range(2)], axis=1)
            hots = jnp.concatenate([hot_rows(both_groups(halo_receive_row, pair, k0 + f), halo_rows) for pair in pairs], axis=1)
            halo_acc[f] += dot_t(sent, hots)

    def edge_phase(layer, q):
        k0 = 2 * q
        for f in range(2):
            latents_copy(layer, k0 + f).wait_recv()
            half_bias = twice(jnp.concatenate([cols[0], cols[0]], axis=0))
            phalo[f] = (dot(w1sr[...], landed[layer, k0 + f]) + half_bias).astype(BF16)
        halo_acc[...] = jnp.zeros_like(halo_acc)

        @pl.loop(0, groups // 2 // UNITS)
        def _(i):
            for slot in range(UNITS + 2 * LAG + SPAN - 1):
                if slot < UNITS:
                    gather_stage(layer, slot, i * UNITS + slot, k0)
                if 0 <= slot - LAG < UNITS:
                    mix_stage(layer, slot - LAG, i * UNITS + slot - LAG, k0)
                done = slot - 2 * LAG + 1
                if 0 < done <= UNITS and done % SPAN == 0:
                    scatter_stage([i * UNITS + u for u in range(done - SPAN, done)], k0)

        for f in range(2):
            hsend[layer, pl.ds(k0 + f, 1)] = halo_acc[f].astype(BF16)[None]
            sums_copy(layer, k0 + f).start()

    def slots(layer, faces, base):
        lane = iota((halo_rows, TILE), 1)
        hots = []
        for j in range(2):
            goal = (lane + (base + j * TILE)).astype(I16)
            hots.append(jnp.concatenate(
                [jnp.where(scol[k * halo_rows:(k + 1) * halo_rows, :].astype(I16) == goal, jnp.ones((), BF16), jnp.zeros((), BF16))
                 for k in faces], axis=0))
        values = jnp.concatenate([returned[layer, k] for k in faces], axis=1)
        return dot(values, jnp.concatenate(hots, axis=1))

    def early_sums(layer, faces):
        for k in faces:
            sums_copy(layer, k).wait_recv()

        @pl.loop(0, own_rows // 256 // CHUNKS)
        def _(c):
            for i in range(CHUNKS):
                pair = c * CHUNKS + i
                extra = slots(layer, faces, pair * 256)
                own_acc[pair * 2] += extra[:, :TILE]
                own_acc[pair * 2 + 1] += extra[:, TILE:]

    def node_mlp(layer, faces):
        for k in faces:
            sums_copy(layer, k).wait_recv()
        sums[...] = jnp.zeros_like(sums)

        @pl.loop(0, own_rows // 256 // CHUNKS)
        def _(c):
            joined, hidden = [], []
            for i in range(CHUNKS):
                pair = c * CHUNKS + i
                own = jnp.concatenate([own_acc[pair * 2], own_acc[pair * 2 + 1]], axis=1)
                agg = (own + slots(layer, faces, pair * 256)).astype(BF16)
                at = pl.ds(pl.multiple_of(pair * 256, 256), 256)
                joined.append(jnp.concatenate([ht[:, at], agg], axis=0))
            for i in range(CHUNKS):
                hidden.append(jnp.maximum(dot(nw1[...], joined[i]) + twice(cols[3]), 0.0).astype(BF16))
            for i in range(CHUNKS):
                update = dot(nw2[...], hidden[i])
                at = pl.ds(pl.multiple_of((c * CHUNKS + i) * 256, 256), 256)
                upd[:, at] = update
                if layer < LAYERS - 1:
                    soon[:, at] = update.astype(BF16)
                square = update * update
                sums[0] += update[:, :TILE] + update[:, TILE:]
                sums[1] += square[:, :TILE] + square[:, TILE:]

        packed = jnp.concatenate([jnp.sum(sums[i].T, axis=0, keepdims=True) for i in range(2)], axis=0)
        mine[layer] = packed
        stats[layer, pl.ds(me, 1)] = packed[None]

        @pl.loop(1, n)
        def _(j):
            stats_copy(layer, j).start()

    def node_norm(layer):
        last = layer == LAYERS - 1
        if last:
            turn_edges()
        else:
            gather_ahead()

        @pl.loop(1, n)
        def _(j):
            stats_copy(layer, j).wait()

        total = jnp.sum(stats[layer], axis=0)
        count = own_rows * n
        mean = total[0:1] / count
        variance = jnp.maximum(total[1:2] / count - mean * mean, 0.0)
        scale = ngain_ref[layer:layer + 1, :] * lax.rsqrt(variance + 1e-05)
        cols[4] = column(scale)
        cols[5] = column(nshift_ref[layer:layer + 1, :] - scale * mean)
        if not last:
            send_next(layer + 1)

        @pl.loop(0, own_rows // 512)
        def _(c):
            for half in range(2):
                at = pl.ds(pl.multiple_of((c * 2 + half) * 256, 256), 256)
                new = (ht[:, at].astype(F32) + twice(cols[4]) * upd[:, at] + twice(cols[5])).astype(BF16)
                if last:
                    hout_ref[at, :] = new.T
                else:
                    ht[:, at] = new

    load_edge_weights(0)
    load_node_weights(0)
    send_first()
    for layer in range(LAYERS):
        own_tables()
        if layer == 0:
            edges_in.wait()

        @pl.loop(0, FACES // 2)
        def _(p):
            edge_phase(layer, face_pair(p))

        early_sums(layer, (0, 1))
        early_sums(layer, (4, 5))
        node_mlp(layer, (2, 3))
        if layer < LAYERS - 1:
            load_edge_weights(layer + 1)
            load_node_weights(layer + 1)
        node_norm(layer)

        @pl.loop(0, FACES)
        def _(k):
            latents_copy(layer, k).wait_send()
            sums_copy(layer, k).wait_send()


def place_kernel(h_in, e_in, h_ref, e_ref, sems):
    parts = sems.shape[0] - 1
    rows = e_in.shape[0] // parts
    copies = [pltpu.make_async_copy(e_in.at[pl.ds(i * rows, rows)], e_ref.at[pl.ds(i * rows, rows)], sems.at[i])
              for i in range(parts)]
    copies.append(pltpu.make_async_copy(h_in, h_ref, sems.at[parts]))
    for copy in copies:
        copy.start()
    for copy in copies:
        copy.wait()


def per_device(n, node_latent, edge_latent, edge_ends, edge_owned, send_index, edge_w1, edge_b1, edge_w2,
               edge_gain, edge_shift, node_w1, node_b1, node_w2, node_gain, node_shift):
    own_rows, width = node_latent.shape
    slots = edge_latent.shape[0]
    halo_rows = send_index.shape[2]
    groups = own_rows // TILE
    vmem = pl.BlockSpec(memory_space=VMEM)
    faces = (LAYERS, FACES, width, halo_rows)
    sems = pltpu.SemaphoreType.DMA((LAYERS, FACES))
    peers = pltpu.SemaphoreType.DMA((LAYERS, n))
    inputs = (node_latent, edge_latent, edge_ends, edge_owned.reshape(1, slots), send_index.reshape(1, FACES * halo_rows),
              edge_w1, edge_b1, edge_w2, edge_gain, edge_shift, node_w1, node_b1, node_w2, node_gain, node_shift)
    inputs = [pltpu.with_memory_space_constraint(a, pltpu.HBM) for a in inputs]
    nodes, edges = pl.pallas_call(
        functools.partial(mesh_kernel, n),
        in_specs=[pl.BlockSpec(memory_space=pltpu.HBM)] * len(inputs),
        out_specs=[vmem, vmem],
        out_shape=[jax.ShapeDtypeStruct((own_rows, width), BF16),
                   jax.ShapeDtypeStruct((groups, FACES, width, TILE), BF16)],
        scratch_shapes=[VMEM(a.shape, a.dtype) for i, a in enumerate(inputs) if i != 1] + [
            VMEM((width, own_rows), BF16), VMEM((width, own_rows), BF16), VMEM((FACES, width, halo_rows), F32),
            VMEM((slots, width), BF16),
            VMEM((UNITS, 2, width, 2 * TILE), BF16),
            VMEM((groups, width, 2 * TILE), BF16),
            VMEM((2, 2 * width, halo_rows), BF16),
            VMEM((groups, width, TILE), F32),
            VMEM((2, width, halo_rows), F32),
            VMEM((width, own_rows), F32),
            VMEM((FACES * halo_rows, TILE), I32),
            VMEM((width, width), BF16),
            VMEM((2 * width, width), BF16),
            VMEM((width, width), BF16),
            VMEM((6, width, TILE), F32),
            VMEM((width, 2 * width), BF16),
            VMEM((width, width), BF16),
            VMEM(faces, BF16), VMEM(faces, BF16), VMEM(faces, BF16), VMEM(faces, BF16),
            VMEM((2, width, TILE), F32), VMEM((LAYERS, 2, width), F32), VMEM((LAYERS, n, 2, width), F32),
            pltpu.SemaphoreType.DMA, pltpu.SemaphoreType.DMA((len(inputs) - 1,)),
            sems, sems, sems, sems, peers, peers,
        ],
        compiler_params=pltpu.CompilerParams(collective_id=0, has_side_effects=True, vmem_limit_bytes=44 * 2 ** 20),
    )(*inputs)
    results = [pltpu.with_memory_space_constraint(a, pltpu.VMEM) for a in (nodes, edges.reshape(slots, width))]
    parts = 6
    return pl.pallas_call(
        place_kernel,
        in_specs=[vmem, vmem],
        out_specs=[pl.BlockSpec(memory_space=pltpu.HBM)] * 2,
        out_shape=[jax.ShapeDtypeStruct((own_rows, width), BF16), jax.ShapeDtypeStruct((slots, width), BF16)],
        scratch_shapes=[pltpu.SemaphoreType.DMA((parts + 1,))],
        compiler_params=pltpu.CompilerParams(vmem_limit_bytes=4 * 2 ** 20),
    )(*results)


def solution(mesh):
    row, rep = P("blk", None), P()
    return jax.shard_map(
        functools.partial(per_device, mesh.shape["blk"]),
        mesh=mesh,
        in_specs=(row, row, P(None, "blk"), P("blk"), P("blk", None, None)) + (rep,) * 10,
        out_specs=(row, row),
        check_vma=False,
    )
```

```python
import functools

import jax
import jax.numpy as jnp
from jax import lax
from jax.experimental import pallas as pl
from jax.experimental.pallas import tpu as pltpu
from jax.sharding import PartitionSpec as P

LAYERS = 2
FACES = 6
GX = 4
GY = 4
TILE = 128
UNITS = 16
LAG = 1
SPAN = 1
CHUNKS = 8
MESH = pl.DeviceIdType.MESH
VMEM = pltpu.VMEM
F32 = jnp.float32
BF16 = jnp.bfloat16
I32 = jnp.int32
I16 = jnp.int16


def dot(a, b):
    return jnp.dot(a, b, preferred_element_type=F32)


def dot_t(a, b):
    return lax.dot_general(a, b, (((1,), (1,)), ((), ())), preferred_element_type=F32)


def iota(shape, axis):
    return lax.broadcasted_iota(I32, shape, axis)


def hot_rows(row, rows):
    width = row.shape[1]
    wide = jnp.broadcast_to(row, (16, width)).astype(I16)
    wide = jnp.concatenate([wide] * (rows // 16), axis=0)
    return jnp.where(wide == iota((rows, width), 0).astype(I16), jnp.ones((), BF16), jnp.zeros((), BF16))


def column(row):
    return jnp.broadcast_to(row, (TILE, TILE)).T


def twice(block):
    return jnp.concatenate([block, block], axis=1)


def face_pair(phase):
    return lax.rem(2 * phase, FACES // 2)


def face_target(me, face, n, sign):
    step = jnp.where(face < 2, 1, jnp.where(face < 4, GX, GX * GY))
    step = jnp.where(face % 2 == 0, step, -step) * sign
    return lax.rem(me + step + n * GX * GY, n)


def mesh_kernel(n, h_in, e_ref, ends_in, owned_in, send_in, ew1_in, eb1_in, ew2_in, egain_in, eshift_in,
                nw1_in, nb1_in, nw2_in, ngain_in, nshift_in,
                hout_ref, et,
                h_ref, ends_ref, owned_ref, send_ref, ew1_ref, eb1_ref, ew2_ref, egain_ref, eshift_ref,
                nw1_ref, nb1_ref, nw2_ref, ngain_ref, nshift_ref,
                ht, soon, ahead, estage, hid, ptab, phalo, own_acc, halo_acc, upd, scol, w1e, w1sr, w2c, cols, nw1, nw2,
                stage, landed, hsend, returned, sums, mine, stats,
                esem, isem, lsend, lrecv, bsend, brecv, tsem, usem):
    inputs = [(h_in, h_ref), (send_in, send_ref), (ew1_in, ew1_ref), (eb1_in, eb1_ref), (ew2_in, ew2_ref),
              (egain_in, egain_ref), (eshift_in, eshift_ref), (nw1_in, nw1_ref), (nb1_in, nb1_ref), (nw2_in, nw2_ref),
              (ngain_in, ngain_ref), (nshift_in, nshift_ref), (ends_in, ends_ref), (owned_in, owned_ref)]
    loads = [pltpu.make_async_copy(source, target, isem.at[i]) for i, (source, target) in enumerate(inputs)]
    for load in loads:
        load.start()
    edges_in = pltpu.make_async_copy(e_ref, estage, esem)
    edges_in.start()
    me = lax.axis_index("blk")
    own_rows, width = h_ref.shape
    halo_rows = stage.shape[3]
    groups = own_rows // TILE
    barrier = pltpu.get_barrier_semaphore()

    @pl.loop(1, n)
    def _(j):
        pl.semaphore_signal(barrier, inc=1, device_id=(lax.rem(me + j, n),), device_id_type=MESH)

    def latents_copy(layer, k):
        return pltpu.make_async_remote_copy(
            src_ref=stage.at[layer, k], dst_ref=landed.at[layer, k], send_sem=lsend.at[layer, k],
            recv_sem=lrecv.at[layer, k], device_id=(face_target(me, k, n, 1),), device_id_type=MESH)

    def sums_copy(layer, k):
        return pltpu.make_async_remote_copy(
            src_ref=hsend.at[layer, k], dst_ref=returned.at[layer, k], send_sem=bsend.at[layer, k],
            recv_sem=brecv.at[layer, k], device_id=(face_target(me, k, n, -1),), device_id_type=MESH)

    def stats_copy(layer, j):
        return pltpu.make_async_remote_copy(
            src_ref=mine.at[layer], dst_ref=stats.at[layer, me], send_sem=tsem.at[layer, j],
            recv_sem=usem.at[layer, j], device_id=(lax.rem(me + j, n),), device_id_type=MESH)

    loads[0].wait()
    for i in range(groups):
        ht[:, i * TILE:(i + 1) * TILE] = h_ref[i * TILE:(i + 1) * TILE, :].T
    for load in loads[1:]:
        load.wait()
    for j in range(FACES * halo_rows // TILE):
        row = send_ref[0:1, j * TILE:(j + 1) * TILE]
        scol[j * TILE:(j + 1) * TILE, :] = column(row)

    def gather(k0, source):
        totals = [None] * 2
        picks = [send_ref[0:1, pl.ds(pl.multiple_of((k0 + f) * halo_rows, TILE), halo_rows)] for f in range(2)]
        for b in range(own_rows // 256):
            for f in range(2):
                part = dot(source[:, b * 256:(b + 1) * 256], hot_rows(picks[f] - b * 256, 256))
                totals[f] = part if totals[f] is None else totals[f] + part
        return totals

    def send_first():
        for phase in range(FACES // 2):
            k0 = 2 * (2 * phase % (FACES // 2))
            totals = gather(k0, ht)
            if phase == 0:
                pl.semaphore_wait(barrier, n - 1)
            for f in range(2):
                stage[0, k0 + f] = totals[f].astype(BF16)
                latents_copy(0, k0 + f).start()

    def gather_ahead():
        @pl.loop(0, FACES // 2)
        def _(q):
            totals = gather(2 * q, soon)
            for f in range(2):
                ahead[2 * q + f] = totals[f]

    def send_next(layer):
        @pl.loop(0, FACES // 2)
        def _(p):
            k0 = 2 * face_pair(p)
            for f in range(2):
                old = stage[layer - 1, k0 + f].astype(F32)
                new = old + twice(cols[4]) * ahead[k0 + f] + twice(cols[5])
                stage[layer, pl.ds(k0 + f, 1)] = new.astype(BF16)[None]
                latents_copy(layer, k0 + f).start()

    def turn_edges():
        @pl.loop(0, groups // 2)
        def _(i):
            turned = [et[i * 2 + g, k].T for g in range(2) for k in range(FACES)]
            for g in range(2):
                for k in range(FACES):
                    et[i * 2 + g, k] = turned[g * FACES + k]

    def load_edge_weights(layer):
        w1e[...] = ew1_ref[layer, 0:width, :].T
        w1sr[0:width, :] = ew1_ref[layer, width:2 * width, :].T
        w1sr[width:2 * width, :] = ew1_ref[layer, 2 * width:3 * width, :].T
        second = ew2_ref[layer].astype(F32).T
        second = second - jnp.mean(second, axis=0, keepdims=True)
        w2c[...] = second.astype(BF16)
        cols[0] = column(0.5 * eb1_ref[layer:layer + 1, :])
        cols[1] = column(egain_ref[layer:layer + 1, :])
        cols[2] = column(eshift_ref[layer:layer + 1, :])

    def load_node_weights(layer):
        nw1[...] = nw1_ref[layer].T
        nw2[...] = nw2_ref[layer].T
        cols[3] = column(nb1_ref[layer:layer + 1, :])

    def own_tables(fresh):
        chunk = 4 * TILE
        parts = 4 if own_rows // chunk % 4 == 0 else 1

        @pl.loop(0, own_rows // chunk // parts)
        def _(c):
            for part in range(parts):
                index = c * parts + part
                at = pl.ds(pl.multiple_of(index * chunk, chunk), chunk)
                nodes = ht[:, at]
                if fresh:
                    scale, offset = [twice(twice(cols[i])) for i in (4, 5)]
                    nodes = (nodes.astype(F32) + scale * upd[:, at] + offset).astype(BF16)
                    ht[:, at] = nodes
                both = dot(w1sr[...], nodes)
                both = (both + twice(twice(jnp.concatenate([cols[0], cols[0]], axis=0)))).astype(BF16)
                for j in range(4):
                    lanes = slice(j * TILE, (j + 1) * TILE)
                    ptab[pl.ds(index * 4 + j, 1)] = jnp.concatenate([both[:width, lanes], both[width:, lanes]], axis=1)[None]
                    own_acc[pl.ds(index * 4 + j, 1)] = jnp.zeros((1, TILE, TILE), F32)

    def ends_of(group, face):
        first = pl.multiple_of((group * FACES + face) * TILE, TILE)
        s = ends_ref[0:1, pl.ds(first, TILE)]
        r = ends_ref[1:2, pl.ds(first, TILE)]
        ok = owned_ref[0:1, pl.ds(first, TILE)] > 0
        return s, r, ok, r >= own_rows

    def both_tiles(pick, group, k0):
        return jnp.concatenate([pick(group, k0), pick(group, k0 + 1)], axis=1)

    def send_row(group, face):
        s, _, _, _ = ends_of(group, face)
        return jnp.where(s >= own_rows, -1, s - group * TILE)

    def receive_row(group, face):
        _, r, ok, r_halo = ends_of(group, face)
        return jnp.where(ok & ~r_halo, r - group * TILE, -1)

    def halo_row(group, face):
        s, r, ok, r_halo = ends_of(group, face)
        return jnp.where(ok, jnp.where(r_halo, r, s) - (own_rows + face * halo_rows), -1)

    def halo_flag(group, face):
        _, _, ok, r_halo = ends_of(group, face)
        return jnp.where(ok & r_halo, 1.0, 0.0)

    def halo_receive_row(group, face):
        _, r, ok, r_halo = ends_of(group, face)
        return jnp.where(ok & r_halo, r - (own_rows + face * halo_rows), -1)

    def both_groups(pick, pair, face):
        return jnp.concatenate([pick(pair * 2, face), pick(pair * 2 + 1, face)], axis=1)

    def gather_stage(layer, u, pair, k0):
        own = []
        for g in range(2):
            group = pair * 2 + g
            old = []
            for f in range(2):
                if layer == 0:
                    first = pl.multiple_of((group * FACES + k0 + f) * TILE, TILE)
                    old.append(estage[pl.ds(first, TILE), :].T)
                    et[group, k0 + f] = old[f]
                else:
                    old.append(et[group, k0 + f])
            hots = jnp.concatenate([hot_rows(both_tiles(send_row, group, k0), TILE),
                                    hot_rows(both_tiles(receive_row, group, k0), TILE),
                                    jnp.concatenate(old, axis=1)], axis=0)
            before = dot(jnp.concatenate([ptab[group], w1e[...]], axis=1), hots)
            own.append(before)
        from_halo = [[None] * 2, [None] * 2]
        for f in range(2):
            both = dot(phalo[f], hot_rows(both_groups(halo_row, pair, k0 + f), halo_rows))
            for g in range(2):
                part = both[:, g * TILE:(g + 1) * TILE]
                flag = jnp.broadcast_to(halo_flag(pair * 2 + g, k0 + f), (width, TILE)) > 0.5
                from_halo[g][f] = jnp.where(flag, part[width:], part[:width])
        for g in range(2):
            before = own[g] + jnp.concatenate(from_halo[g], axis=1)
            hid[u, g] = jnp.maximum(before, 0.0).astype(BF16)

    def mix_stage(layer, u, pair, k0):
        for g in range(2):
            group = pair * 2 + g
            centre = dot(w2c[...], hid[u, g])
            spread = jnp.mean(centre * centre, axis=0, keepdims=True)
            ok = jnp.concatenate([owned_ref[0:1, pl.ds(pl.multiple_of((group * FACES + k0 + f) * TILE, TILE), TILE)]
                                  for f in range(2)], axis=1)
            keep = jnp.broadcast_to(ok, centre.shape) > 0
            normed = twice(cols[1]) * (centre * lax.rsqrt(spread + 1e-05)) + twice(cols[2])
            old = jnp.concatenate([et[group, k0], et[group, k0 + 1]], axis=1)
            new = (old.astype(F32) + jnp.where(keep, normed, 0.0)).astype(BF16)
            for f in range(2):
                et[group, k0 + f] = new[:, f * TILE:(f + 1) * TILE]

    def scatter_stage(pairs, k0):
        for pair in pairs:
            for g in range(2):
                group = pair * 2 + g
                new = jnp.concatenate([et[group, k0], et[group, k0 + 1]], axis=1)
                own_acc[group] += dot_t(new, hot_rows(both_tiles(receive_row, group, k0), TILE))
        for f in range(2):
            sent = jnp.concatenate([et[pair * 2 + g, k0 + f] for pair in pairs for g in range(2)], axis=1)
            hots = jnp.concatenate([hot_rows(both_groups(halo_receive_row, pair, k0 + f), halo_rows) for pair in pairs], axis=1)
            halo_acc[f] += dot_t(sent, hots)

    def edge_phase(layer, q):
        k0 = 2 * q
        for f in range(2):
            latents_copy(layer, k0 + f).wait_recv()
            half_bias = twice(jnp.concatenate([cols[0], cols[0]], axis=0))
            phalo[f] = (dot(w1sr[...], landed[layer, k0 + f]) + half_bias).astype(BF16)
        halo_acc[...] = jnp.zeros_like(halo_acc)

        @pl.loop(0, groups // 2 // UNITS)
        def _(i):
            for slot in range(UNITS + 2 * LAG + SPAN - 1):
                if slot < UNITS:
                    gather_stage(layer, slot, i * UNITS + slot, k0)
                if 0 <= slot - LAG < UNITS:
                    mix_stage(layer, slot - LAG, i * UNITS + slot - LAG, k0)
                done = slot - 2 * LAG + 1
                if 0 < done <= UNITS and done % SPAN == 0:
                    scatter_stage([i * UNITS + u for u in range(done - SPAN, done)], k0)

        for f in range(2):
            hsend[layer, pl.ds(k0 + f, 1)] = halo_acc[f].astype(BF16)[None]
            sums_copy(layer, k0 + f).start()

    def slots(layer, faces, base):
        lane = iota((halo_rows, TILE), 1)
        hots = []
        for j in range(2):
            goal = (lane + (base + j * TILE)).astype(I16)
            hots.append(jnp.concatenate(
                [jnp.where(scol[k * halo_rows:(k + 1) * halo_rows, :].astype(I16) == goal, jnp.ones((), BF16), jnp.zeros((), BF16))
                 for k in faces], axis=0))
        values = jnp.concatenate([returned[layer, k] for k in faces], axis=1)
        return dot(values, jnp.concatenate(hots, axis=1))

    def early_sums(layer, faces):
        for k in faces:
            sums_copy(layer, k).wait_recv()

        @pl.loop(0, own_rows // 256 // CHUNKS)
        def _(c):
            for i in range(CHUNKS):
                pair = c * CHUNKS + i
                extra = slots(layer, faces, pair * 256)
                own_acc[pair * 2] += extra[:, :TILE]
                own_acc[pair * 2 + 1] += extra[:, TILE:]

    def node_mlp(layer, faces):
        for k in faces:
            sums_copy(layer, k).wait_recv()
        sums[...] = jnp.zeros_like(sums)

        @pl.loop(0, own_rows // 256 // CHUNKS)
        def _(c):
            joined, hidden = [], []
            for i in range(CHUNKS):
                pair = c * CHUNKS + i
                own = jnp.concatenate([own_acc[pair * 2], own_acc[pair * 2 + 1]], axis=1)
                agg = (own + slots(layer, faces, pair * 256)).astype(BF16)
                at = pl.ds(pl.multiple_of(pair * 256, 256), 256)
                joined.append(jnp.concatenate([ht[:, at], agg], axis=0))
            for i in range(CHUNKS):
                hidden.append(jnp.maximum(dot(nw1[...], joined[i]) + twice(cols[3]), 0.0).astype(BF16))
            for i in range(CHUNKS):
                update = dot(nw2[...], hidden[i])
                at = pl.ds(pl.multiple_of((c * CHUNKS + i) * 256, 256), 256)
                upd[:, at] = update
                if layer < LAYERS - 1:
                    soon[:, at] = update.astype(BF16)
                square = update * update
                sums[0] += update[:, :TILE] + update[:, TILE:]
                sums[1] += square[:, :TILE] + square[:, TILE:]

        packed = jnp.concatenate([jnp.sum(sums[i].T, axis=0, keepdims=True) for i in range(2)], axis=0)
        mine[layer] = packed
        stats[layer, pl.ds(me, 1)] = packed[None]

        @pl.loop(1, n)
        def _(j):
            stats_copy(layer, j).start()

    def node_norm(layer):
        last = layer == LAYERS - 1
        if last:
            turn_edges()
        else:
            gather_ahead()

        @pl.loop(1, n)
        def _(j):
            stats_copy(layer, j).wait()

        total = jnp.sum(stats[layer], axis=0)
        count = own_rows * n
        mean = total[0:1] / count
        variance = jnp.maximum(total[1:2] / count - mean * mean, 0.0)
        scale = ngain_ref[layer:layer + 1, :] * lax.rsqrt(variance + 1e-05)
        cols[4] = column(scale)
        cols[5] = column(nshift_ref[layer:layer + 1, :] - scale * mean)
        if not last:
            send_next(layer + 1)
            return

        @pl.loop(0, own_rows // 512)
        def _(c):
            for half in range(2):
                at = pl.ds(pl.multiple_of((c * 2 + half) * 256, 256), 256)
                new = ht[:, at].astype(F32) + twice(cols[4]) * upd[:, at] + twice(cols[5])
                hout_ref[at, :] = new.astype(BF16).T

    load_edge_weights(0)
    load_node_weights(0)
    send_first()
    for layer in range(LAYERS):
        own_tables(layer > 0)
        if layer == 0:
            edges_in.wait()

        @pl.loop(0, FACES // 2)
        def _(p):
            edge_phase(layer, face_pair(p))

        early_sums(layer, (0, 1))
        early_sums(layer, (4, 5))
        node_mlp(layer, (2, 3))
        if layer < LAYERS - 1:
            load_edge_weights(layer + 1)
            load_node_weights(layer + 1)
        node_norm(layer)

        @pl.loop(0, FACES)
        def _(k):
            latents_copy(layer, k).wait_send()
            sums_copy(layer, k).wait_send()


def place_kernel(h_in, e_in, h_ref, e_ref, sems):
    parts = sems.shape[0] - 1
    rows = e_in.shape[0] // parts
    copies = [pltpu.make_async_copy(e_in.at[pl.ds(i * rows, rows)], e_ref.at[pl.ds(i * rows, rows)], sems.at[i])
              for i in range(parts)]
    copies.append(pltpu.make_async_copy(h_in, h_ref, sems.at[parts]))
    for copy in copies:
        copy.start()
    for copy in copies:
        copy.wait()


def per_device(n, node_latent, edge_latent, edge_ends, edge_owned, send_index, edge_w1, edge_b1, edge_w2,
               edge_gain, edge_shift, node_w1, node_b1, node_w2, node_gain, node_shift):
    own_rows, width = node_latent.shape
    slots = edge_latent.shape[0]
    halo_rows = send_index.shape[2]
    groups = own_rows // TILE
    vmem = pl.BlockSpec(memory_space=VMEM)
    faces = (LAYERS, FACES, width, halo_rows)
    sems = pltpu.SemaphoreType.DMA((LAYERS, FACES))
    peers = pltpu.SemaphoreType.DMA((LAYERS, n))
    inputs = (node_latent, edge_latent, edge_ends, edge_owned.reshape(1, slots), send_index.reshape(1, FACES * halo_rows),
              edge_w1, edge_b1, edge_w2, edge_gain, edge_shift, node_w1, node_b1, node_w2, node_gain, node_shift)
    inputs = [pltpu.with_memory_space_constraint(a, pltpu.HBM) for a in inputs]
    nodes, edges = pl.pallas_call(
        functools.partial(mesh_kernel, n),
        in_specs=[pl.BlockSpec(memory_space=pltpu.HBM)] * len(inputs),
        out_specs=[vmem, vmem],
        out_shape=[jax.ShapeDtypeStruct((own_rows, width), BF16),
                   jax.ShapeDtypeStruct((groups, FACES, width, TILE), BF16)],
        scratch_shapes=[VMEM(a.shape, a.dtype) for i, a in enumerate(inputs) if i != 1] + [
            VMEM((width, own_rows), BF16), VMEM((width, own_rows), BF16), VMEM((FACES, width, halo_rows), F32),
            VMEM((slots, width), BF16),
            VMEM((UNITS, 2, width, 2 * TILE), BF16),
            VMEM((groups, width, 2 * TILE), BF16),
            VMEM((2, 2 * width, halo_rows), BF16),
            VMEM((groups, width, TILE), F32),
            VMEM((2, width, halo_rows), F32),
            VMEM((width, own_rows), F32),
            VMEM((FACES * halo_rows, TILE), I32),
            VMEM((width, width), BF16),
            VMEM((2 * width, width), BF16),
            VMEM((width, width), BF16),
            VMEM((6, width, TILE), F32),
            VMEM((width, 2 * width), BF16),
            VMEM((width, width), BF16),
            VMEM(faces, BF16), VMEM(faces, BF16), VMEM(faces, BF16), VMEM(faces, BF16),
            VMEM((2, width, TILE), F32), VMEM((LAYERS, 2, width), F32), VMEM((LAYERS, n, 2, width), F32),
            pltpu.SemaphoreType.DMA, pltpu.SemaphoreType.DMA((len(inputs) - 1,)),
            sems, sems, sems, sems, peers, peers,
        ],
        compiler_params=pltpu.CompilerParams(collective_id=0, has_side_effects=True, vmem_limit_bytes=44 * 2 ** 20),
    )(*inputs)
    results = [pltpu.with_memory_space_constraint(a, pltpu.VMEM) for a in (nodes, edges.reshape(slots, width))]
    parts = 6
    return pl.pallas_call(
        place_kernel,
        in_specs=[vmem, vmem],
        out_specs=[pl.BlockSpec(memory_space=pltpu.HBM)] * 2,
        out_shape=[jax.ShapeDtypeStruct((own_rows, width), BF16), jax.ShapeDtypeStruct((slots, width), BF16)],
        scratch_shapes=[pltpu.SemaphoreType.DMA((parts + 1,))],
        compiler_params=pltpu.CompilerParams(vmem_limit_bytes=4 * 2 ** 20),
    )(*results)


def solution(mesh):
    row, rep = P("blk", None), P()
    return jax.shard_map(
        functools.partial(per_device, mesh.shape["blk"]),
        mesh=mesh,
        in_specs=(row, row, P(None, "blk"), P("blk"), P("blk", None, None)) + (rep,) * 10,
        out_specs=(row, row),
        check_vma=False,
    )
```
